32 devices in a mesh: row: 8 (over z, y), col: 4 (over x, core).
Axes of the slice: x: 2, y: 2, z: 4, core: 2. Of those that a mesh axis runs over, the one named last changes fastest.
Arguments:
- moment: bfloat16 [2, 4096, 4096], P(None, 'row', 'col'), may hold values from -6 to 6
- second: float32 [2, 4096, 4096], P(None, 'row', 'col'), may hold values from 0.04 to 2
- left_old: bfloat16 [2, 4096, 4096], P(None, 'col', 'row'), may hold values from -0.09375 to 0.09375
- left_new: bfloat16 [2, 4096, 4096], P(None, 'col', 'row'), may hold values from -0.09375 to 0.09375
- right_old: bfloat16 [4096, 4096], P('row', 'col'), may hold values from -0.09375 to 0.09375
- right_new: bfloat16 [4096, 4096], P('row', 'col'), may hold values from -0.09375 to 0.09375
Outputs:
- moment_new: bfloat16 [2, 4096, 4096], P(None, 'row', 'col')
- direction: bfloat16 [2, 4096, 4096], P(None, 'row', 'col')
The draws below stay inside these ranges and needn't reach their ends.
All inputs are finite; a program needn't handle non-finite values.
Results may differ from the reference program's by a relative error of at most 0.03.
Values may be sent and summed in bfloat16 or wider, within the bound.
No kernel may reach another device: no remote copies, remote signals or barrier semaphores. Data moves between devices by JAX's collectives and lax.ppermute only.
A program may use at most 128 MiB of HBM per device.

```python
import math
import jax
import jax.numpy as jnp
from jax import lax

LBLK = 4096
RW = 4096
NBLK = 2
N_ROW = 8
N_COL = 4


def levels(own_key, dims, cuts, low, top_value):
    factor_of = 1.0
    for dim, parts in cuts:
        steps = jax.random.uniform(jax.random.fold_in(jax.random.fold_in(own_key, 6), dim), (parts,), jnp.float32, low / len(cuts), top_value / len(cuts))
        factor_of = factor_of * jnp.repeat(jnp.exp(steps), dims[dim] // parts).reshape((-1,) + (1,) * (len(dims) - 1 - dim))
    return factor_of


def gaussian(stream_key, dims, width, reach, split=(), kind=jnp.bfloat16):
    array = width * jax.random.normal(stream_key, dims, jnp.float32)
    if split:
        array = array * levels(stream_key, dims, split, -0.22, 0.18)
    return jnp.clip(array, -reach, reach).astype(kind)


def setup_inputs(seed: int = 0) -> dict:
    streams_of = jax.random.split(jax.random.key(seed), 7)
    return {
        "moment": gaussian(streams_of[0], (NBLK, LBLK, RW), 1.0, 6.0, ((1, 8), (2, 4))),
        "second": jnp.clip(jnp.exp(math.log(2.0) - 3.912023 * jax.random.uniform(streams_of[1], (NBLK, LBLK, RW), jnp.float32) ** levels(streams_of[1], (NBLK, LBLK, RW), ((1, 8), (2, 4)), -0.2, 0.2)), 0.04, 2.0),
        "left_old": gaussian(streams_of[2], (NBLK, LBLK, LBLK), LBLK ** -0.5, 0.09375, ((1, 4), (2, 8))),
        "left_new": gaussian(streams_of[3], (NBLK, LBLK, LBLK), LBLK ** -0.5, 0.09375, ((1, 4), (2, 8))),
        "right_old": gaussian(streams_of[4], (RW, RW), RW ** -0.5, 0.09375, ((0, 8), (1, 4))),
        "right_new": gaussian(streams_of[5], (RW, RW), RW ** -0.5, 0.09375, ((0, 8), (1, 4))),
    }


def grouped_product(new_basis, old_basis, groups):
    group_rows = new_basis.shape[0] // groups

    def accumulate(running, group_index):
        offset = (group_index * group_rows).astype(jnp.int32)
        new_part = lax.dynamic_slice_in_dim(new_basis, offset, group_rows, 0)
        old_part = lax.dynamic_slice_in_dim(old_basis, offset, group_rows, 0)
        partial_sum = jnp.dot(new_part.T, old_part, preferred_element_type=jnp.float32)
        rounded = lax.optimization_barrier(partial_sum.astype(jnp.bfloat16))
        return (running + rounded.astype(jnp.float32), None)
    start_sum = jnp.zeros((new_basis.shape[1], old_basis.shape[1]), jnp.float32)
    running, unused = lax.scan(accumulate, start_sum, jnp.arange(groups, dtype=jnp.int32))
    return running.astype(jnp.bfloat16)

def reference(moment, second, left_old, left_new, right_old, right_new):
    right_transition = grouped_product(right_new, right_old, N_ROW)

    def one_block(inputs):
        block_moment, block_old, block_new = inputs
        left_transition = grouped_product(block_new, block_old, N_COL)
        rotated = jnp.dot(left_transition, block_moment, preferred_element_type=jnp.float32).astype(jnp.bfloat16)
        return jnp.dot(rotated, right_transition.T, preferred_element_type=jnp.float32).astype(jnp.bfloat16)
    moment_new = lax.map(one_block, (moment, left_old, left_new))
    direction = (moment_new.astype(jnp.float32) / (jnp.sqrt(second) + 1e-08)).astype(jnp.bfloat16)
    return (moment_new, direction)
```

```python
import jax
import jax.numpy as jnp
from jax import lax
from jax.sharding import PartitionSpec as P

F32 = jnp.float32
BF16 = jnp.bfloat16
CHUNKS = 2


class Grid:
    def __init__(self, rows, cols, ny):
        self.rows, self.cols, self.ny = rows, cols, ny
        depth = rows // ny
        bits = depth.bit_length() - 1
        self.nb = 1 << (bits // 2)
        self.na = depth // self.nb
        self.nc = 2 if cols % 2 == 0 else 1
        self.nx = cols // self.nc
        row, col = lax.axis_index("row"), lax.axis_index("col")
        z, self.y = row // ny, row % ny
        gray = z ^ (z >> 1)
        self.a, self.b = gray // self.nb, gray % self.nb
        self.x, self.c = col // self.nc, col % self.nc

    def row_bits(self, row):
        z, y = divmod(row, self.ny)
        gray = z ^ (z >> 1)
        return {"a": gray // self.nb, "b": gray % self.nb, "y": y}

    def send(self, value, group, shift):
        if group in ("x", "c"):
            step = shift * self.nc if group == "x" else shift
            return lax.ppermute(value, "col", [(s, s ^ step) for s in range(self.cols)])
        place = {}
        for row in range(self.rows):
            bits = self.row_bits(row)
            place[bits["a"], bits["b"], bits["y"]] = row
        pairs = []
        for row in range(self.rows):
            bits = self.row_bits(row)
            bits[group] ^= shift
            pairs.append((row, place[bits["a"], bits["b"], bits["y"]]))
        return lax.ppermute(value, "row", pairs)


def piece(value, index, count, axis):
    size = value.shape[axis] // count
    return lax.dynamic_slice_in_dim(value, index * size, size, axis)


def pick(value, index):
    return lax.dynamic_index_in_dim(value, index, 0, keepdims=False)


def product(lhs, rhs, dims):
    return lax.dot_general(lhs, rhs, (dims, ((), ())), preferred_element_type=F32)


def gather(grid, value, group, count):
    return [value] + [grid.send(value, group, d) for d in range(1, count)]


def transition_right(g, right_old, right_new):
    mine = [piece(right_old, g.b ^ d, g.nb, 1) for d in range(g.nb)]
    old = jnp.concatenate([mine[0]] + [g.send(mine[d], "b", d) for d in range(1, g.nb)], 0)
    old = gather(g, old, "x", g.nx)
    old = [gather(g, o, "c", g.nc) for o in old]
    old = jnp.concatenate([o for group in old for o in group], 1)
    parts = g.na * g.ny
    new = jnp.concatenate(
        [piece(right_new, (g.a ^ da) * g.ny + (g.y ^ dy), parts, 1) for da in range(g.na) for dy in range(g.ny)], 1
    )
    new = jnp.concatenate(gather(g, new, "b", g.nb), 0)
    part = product(new, old, ((0,), (0,)))
    width = old.shape[1]
    part = part.astype(BF16).reshape(g.na, g.ny, -1, width)
    total = part[:, 0].astype(F32)
    for d in range(1, g.ny):
        total = total + g.send(part[:, d], "y", d).astype(F32)
    total = total.astype(BF16)
    mine = total[0].astype(F32)
    for d in range(1, g.na):
        mine = mine + g.send(total[d], "a", d).astype(F32)
    mine = mine.astype(BF16)
    full = jnp.stack(gather(g, mine, "a", g.na))
    full = jnp.stack(gather(g, full, "y", g.ny), 1)
    full = full.reshape(parts, -1, width)
    order = [(p // g.ny ^ g.a) * g.ny + (p % g.ny ^ g.y) for p in range(parts)]
    full = jnp.concatenate([pick(full, o) for o in order], 0)
    both = [full]
    for d in range(1, g.nc):
        other = g.send(full, "c", d).reshape(full.shape[0], g.nx, g.nc, -1)
        both.append(other[:, :, [e ^ d for e in range(g.nc)]].reshape(full.shape))
    return jnp.concatenate(both, 0)


def gather_left_old(g, left_old, d):
    mine = [piece(pick(left_old, g.y ^ e), g.x ^ d, g.nx, 1) for e in range(g.ny)]
    rows = [mine[0]] + [g.send(mine[e], "y", e) for e in range(1, g.ny)]
    rows = jnp.concatenate(rows, 1)
    wide = gather(g, rows, "a", g.na)
    wide = [gather(g, w, "c", g.nc) for w in wide]
    return jnp.concatenate([jnp.concatenate([w[e] for w in wide], 1) for e in range(g.nc)], 0)


def gather_moment(g, moment):
    out = []
    for db in reversed(range(g.nb)):
        cols = piece(moment, g.b ^ db, g.nb, 2)
        rows = []
        for e in range(g.ny):
            own = pick(cols, g.y ^ e)
            own = jnp.stack([piece(own, g.x ^ d, g.nx, 0) for d in range(g.nx)])
            rows.append(g.send(own, "y", e) if e else own)
        rows = jnp.stack(rows, 1)
        wide = jnp.stack(gather(g, rows, "a", g.na), 1)
        wide = wide.reshape(-1, wide.shape[-1])
        out.append(jnp.concatenate(gather(g, wide, "c", g.nc), 1))
    return out[::-1]


def local(rows, cols, moment, second, left_old, left_new, right_old, right_new):
    g = Grid(rows, cols, moment.shape[0])
    own = piece(left_new, g.c, g.nc, 2)
    mine = [own] + [g.send(piece(left_new, g.c ^ d, g.nc, 2), "c", d) for d in range(1, g.nc)]
    new = jnp.concatenate(mine, 1)
    old = {d: gather_left_old(g, left_old, d) for d in reversed(range(g.nx))}
    moments = gather_moment(g, moment)
    right = transition_right(g, right_old, right_new)
    step = new.shape[2] // CHUNKS
    results = []
    for chunk in range(CHUNKS):
        cut = new[:, :, chunk * step : (chunk + 1) * step]
        fresh = [pick(cut, g.y)] + [g.send(pick(cut, g.y ^ e), "y", e) for e in range(1, g.ny)]
        fresh = jnp.concatenate(fresh, 1)
        fresh = jnp.concatenate(gather(g, fresh, "b", g.nb), 1)
        terms = {}
        for d in reversed(range(1, g.nx)):
            terms[d] = g.send(product(fresh, old[d], ((0,), (0,))).astype(BF16), "x", d)
        total = product(fresh, old[0], ((0,), (0,)))
        for d in range(1, g.nx):
            total = total + terms[d].astype(F32)
        total = total.astype(BF16)
        left = jnp.concatenate(gather(g, total, "x", g.nx), 1)
        terms = {}
        for d in reversed(range(1, g.nb)):
            term = product(left, moments[d], ((1,), (0,))).astype(BF16)
            terms[d] = g.send(term, "b", d)
        total = product(left, moments[0], ((1,), (0,)))
        for d in range(1, g.nb):
            term = terms[d].reshape(g.nb, -1, total.shape[1])
            term = jnp.concatenate([term[e ^ d] for e in range(g.nb)], 0)
            total = total + term.astype(F32)
        rotated = jnp.concatenate(gather(g, total.astype(BF16), "x", g.nx), 1)
        rotated = rotated.reshape(g.nb, -1, rotated.shape[1])
        terms = {}
        for d in reversed(range(1, g.nb)):
            terms[d] = g.send(product(rotated[d], right, ((1,), (1,))).astype(BF16), "b", d)
        total = product(rotated[0], right, ((1,), (1,)))
        for d in range(1, g.nb):
            total = total + terms[d].astype(F32)
        total = total.astype(BF16).reshape(g.ny, step, g.nc, -1)
        blocks = [total[0]] + [g.send(total[d], "y", d) for d in range(1, g.ny)]
        halves = []
        for d in range(g.nc):
            half = jnp.stack([block[:, d] for block in blocks])
            halves.append(g.send(half, "c", d) if d else half)
        results.append(jnp.stack(halves, 1))
    result = jnp.stack(results, 2)
    shape = result.shape
    result = jnp.concatenate([piece(result, b ^ g.y, g.ny, 0) for b in range(g.ny)], 0)
    result = jnp.concatenate([piece(result, c ^ g.c, g.nc, 1) for c in range(g.nc)], 1)
    moment_new = result.reshape(second.shape)
    direction = (moment_new.astype(F32) / (jnp.sqrt(second) + 1e-08)).astype(BF16)
    return (moment_new, direction)


def solution(mesh):
    rows, cols = mesh.shape["row"], mesh.shape["col"]

    def body(*args):
        return local(rows, cols, *args)

    return jax.shard_map(
        body,
        mesh=mesh,
        in_specs=(
            P(None, "row", "col"),
            P(None, "row", "col"),
            P(None, "col", "row"),
            P(None, "col", "row"),
            P("row", "col"),
            P("row", "col"),
        ),
        out_specs=(P(None, "row", "col"), P(None, "row", "col")),
        check_vma=False,
    )
```
